32 devices in a mesh: expert: 4 (over z), tp: 8 (over y, x, core).
Axes of the slice: x: 2, y: 2, z: 4, core: 2. Of those that a mesh axis runs over, the one named last changes fastest.
Arguments:
- tokens: bfloat16 [512, 4096], P('expert', 'tp'), may hold values from -6 to 6
- norm_gain: bfloat16 [4096], replicated, may hold values from 0.5 to 1.5
- route_logits: float32 [512, 2], P('expert'), may hold values from -6 to 6
- expert_ids: int32 [512, 2], P('expert'), may hold values from 0 to 3, all different within a row; in each aligned block of 128 rows (0 to 127, 128 to 255, ...) at most 64 rows name the same one
- active: int32 [512], P('expert'), may hold values 0 or 1
- gate_weight: bfloat16 [4, 14336, 4096], P('expert', 'tp'), may hold values from -0.09375 to 0.09375
- up_weight: bfloat16 [4, 14336, 4096], P('expert', 'tp'), may hold values from -0.09375 to 0.09375
- down_weight: bfloat16 [4, 14336, 4096], P('expert', 'tp'), may hold values from -0.046875 to 0.046875
Outputs:
- mixed: bfloat16 [512, 4096], P('expert', 'tp')
The draws below stay inside these ranges and needn't reach their ends.
Inputs may be any that keep to these rules, and one draw needn't show every extreme that they name: `expert_ids`: each token names 2 different experts. In each block of 128 consecutive token slots (the slots of one index of expert) no expert is named by more than 64 tokens, a bound that some block reaches. `active`: each entry is 0 or 1.
All inputs are finite; a program needn't handle non-finite values.
Results may differ from the reference program's by a relative error of at most 0.0025.
Values may be sent and summed in bfloat16 or wider, within the bound.
A program may use at most 128 MiB of HBM per device.

```python
import math
import jax
import jax.numpy as jnp
import numpy as np
from jax import lax

D = 4096
FF = 14336
TOP = 2
WORDS_PER_GROUP = 128
EXPERTS = 4
TOKENS = 512
CAP = 64


def with_ends(result, rng, low, high):
    extent = result.shape
    place = [jax.random.randint(jax.random.fold_in(rng, axis), (), 0, extent[axis]) for axis in range(len(extent))]
    result = result.at[tuple(place)].set(low)
    longest = extent.index(max(extent))
    place[longest] = (place[longest] + 1) % extent[longest]
    return result.at[tuple(place)].set(high)


def strengthened(array, rng, source, target, blocks, factor):
    def block_of(axis_at):
        return (jnp.arange(array.shape[axis_at]) // (array.shape[axis_at] // blocks)).reshape((-1,) + (1,) * (array.ndim - 1 - axis_at))

    first = jax.random.permutation(rng, blocks)[block_of(target)]
    other_side = (block_of(target) + blocks // 2) % blocks
    return jnp.where((block_of(source) == first) | (block_of(source) == other_side), factor * array, array)


def steps_of(own_key, dims, cuts, smallest, high):
    factor_of = 1.0
    for axis_at, blocks in cuts:
        steps = jax.random.uniform(jax.random.fold_in(jax.random.fold_in(own_key, 6), axis_at), (blocks,), jnp.float32, smallest / len(cuts), high / len(cuts))
        factor_of = factor_of * jnp.repeat(jnp.exp(steps), dims[axis_at] // blocks).reshape((-1,) + (1,) * (len(dims) - 1 - axis_at))
    return factor_of


def deal_out(rng, own, number, rows, amount, top, most, slope):
    ranking = jax.random.permutation(rng, amount)
    heavy_load, ordinary = load_shares(amount, rows * top, most, slope, True), load_shares(amount, rows * top, most, slope, False)
    places = jnp.arange(amount)

    def named(lengths, turn):
        used = int((lengths > 0).sum())
        fixed = max(1, used // 4)
        moved = fixed + (places - fixed + turn * (used - fixed)) % max(1, amount - fixed)
        return jnp.zeros((amount,), jnp.int32).at[ranking[jnp.where(places < fixed, places, moved)]].set(jnp.asarray(lengths, jnp.int32))

    lengths = jnp.where(number % 4 == 0, named(heavy_load, number // 4), named(ordinary, number - number // 4 - 1))
    mixed = jax.random.permutation(jax.random.fold_in(own, 3), amount)
    donor, receiver = mixed[0:amount // 2 * 2:2], mixed[1:amount // 2 * 2:2]
    slack = jnp.minimum(lengths[donor] - 1, most - lengths[receiver]) // 2
    slack = jnp.where((donor == ranking[0]) | (receiver == ranking[0]) | (lengths[receiver] == 0), 0, jnp.maximum(slack, 0))
    moved = jax.random.randint(jax.random.fold_in(own, 4), (amount // 2,), 0, 1 << 20) % (slack + 1)
    lengths = lengths.at[donor].add(-moved).at[receiver].add(moved)
    members = jnp.searchsorted(jnp.cumsum(lengths), jnp.arange(rows * top), side="right").astype(jnp.int32)
    grid = members.reshape(top, rows).T
    grid = grid[jax.random.permutation(jax.random.fold_in(own, 1), rows)]
    turn = jax.random.randint(jax.random.fold_in(own, 2), (rows, 1), 0, top)
    return jnp.take_along_axis(grid, (jnp.arange(top)[None, :] + turn) % top, axis=1)


def load_shares(amount, total, bound, lean, full):
    portions = [(1 << 20) // math.isqrt(standing ** lean) + 1 for standing in range(1, amount + 1)]
    largest = bound if full else min(bound, max(-(-total // amount), total * portions[0] // sum(portions)))
    least = 1 if total - largest >= amount - 1 else 0
    holding, surplus = [largest] + [least] * (amount - 1), total - largest - least * (amount - 1)
    while surplus > 0:
        candidates = [i for i in range(1, amount) if holding[i] < largest] or [i for i in range(1, amount) if holding[i] < bound]
        mass, left = sum([portions[i] for i in candidates]), surplus
        for i in candidates:
            addition = min(bound - holding[i], max(1, left * portions[i] // mass), surplus)
            holding[i] = holding[i] + addition
            surplus = surplus - addition
    return np.array(holding)


def noise(rng, dims, width, reach, pieces=(), held_as=jnp.bfloat16):
    array = width * jax.random.normal(rng, dims, jnp.float32)
    if pieces:
        array = array * steps_of(rng, dims, pieces, -0.22, 0.18)
    return jnp.clip(array, -reach, reach).astype(held_as)


def bell_draw_with(rng, shape, spread, reach, cuts, heavy, held_as=jnp.bfloat16):
    values = spread * jax.random.normal(rng, shape, jnp.float32)
    if cuts:
        values = values * steps_of(rng, shape, cuts, -0.22, 0.18)
    return jnp.clip(strengthened(values, jax.random.fold_in(rng, 3), *heavy), -reach, reach).astype(held_as)


def setup_inputs(seed: int = 0) -> dict:
    streams_of = jax.random.split(jax.random.key(seed), 9)
    tokens = bell_draw_with(streams_of[0], (TOKENS, D), 1.0, 6.0, ((0, 4), (1, 8)), (1, 0, 8, 2.0))
    norm_gain = jnp.clip(1.0 + 0.1 * jax.random.normal(streams_of[1], (D,), jnp.float32), 0.5, 1.5).astype(jnp.bfloat16)
    route_logits = noise(streams_of[2], (TOKENS, TOP), 1.0, 6.0, ((0, 4),), jnp.float32)
    expert_ids_keys = jax.random.split(jax.random.fold_in(streams_of[3], 1), TOKENS // WORDS_PER_GROUP)
    expert_ids_turns = jax.random.permutation(jax.random.fold_in(streams_of[3], 3), TOKENS // WORDS_PER_GROUP)
    expert_ids = jax.vmap(lambda own, number: deal_out(jax.random.fold_in(streams_of[3], 2), own, number, WORDS_PER_GROUP, EXPERTS, TOP, CAP, 2))(expert_ids_keys, expert_ids_turns).reshape((TOKENS, TOP))
    active = with_ends((jax.random.randint(streams_of[4], (TOKENS,), 0, 4) < 3).astype(jnp.int32), jax.random.fold_in(streams_of[4], 1), 0, 1)
    gate_weight = noise(streams_of[5], (EXPERTS, FF, D), D ** -0.5, 0.09375, ((0, 4), (1, 8)))
    up_weight = noise(streams_of[6], (EXPERTS, FF, D), D ** -0.5, 0.09375, ((0, 4), (1, 8)))
    down_weight = noise(streams_of[7], (EXPERTS, FF, D), FF ** -0.5, 0.046875, ((0, 4), (1, 8)))
    return dict(tokens=tokens, norm_gain=norm_gain, route_logits=route_logits, expert_ids=expert_ids, active=active, gate_weight=gate_weight, up_weight=up_weight, down_weight=down_weight)


epsilon = 1e-05

def reference(tokens, norm_gain, route_logits, expert_ids, active, gate_weight, up_weight, down_weight):
    widened = tokens.astype(jnp.float32)
    mean_square = lax.optimization_barrier(jnp.sum(widened * widened, axis=1, keepdims=True)) / D
    normed = (widened * lax.rsqrt(mean_square + epsilon) * norm_gain.astype(jnp.float32)).astype(jnp.bfloat16)
    route_probs = jax.nn.softmax(route_logits, axis=1) * active.astype(jnp.float32)[:, None]

    def expert_step(combined, inputs):
        specialist_number, gate_rows, up_rows, down_rows = inputs
        gate_sum = jnp.dot(normed, gate_rows.T, preferred_element_type=jnp.float32)
        up_sum = jnp.dot(normed, up_rows.T, preferred_element_type=jnp.float32)
        inner_width = (jax.nn.silu(gate_sum) * up_sum).astype(jnp.bfloat16)
        output = jnp.dot(inner_width, down_rows, preferred_element_type=jnp.float32).astype(jnp.bfloat16)
        weight = lax.optimization_barrier(jnp.sum(jnp.where(expert_ids == specialist_number, route_probs, jnp.zeros_like(route_probs)), axis=1))
        return (combined + weight[:, None] * output.astype(jnp.float32), None)
    start_value = jnp.zeros(tokens.shape, jnp.float32)
    expert_list = jnp.arange(EXPERTS, dtype=jnp.int32)
    combined, _ = lax.scan(expert_step, start_value, (expert_list, gate_weight, up_weight, down_weight))
    return combined.astype(jnp.bfloat16)
```

```python
import functools

import jax
import jax.numpy as jnp
from jax import lax
from jax.experimental import pallas as pl
from jax.experimental.pallas import tpu as pltpu
from jax.sharding import PartitionSpec as P

epsilon = 1e-05
F32 = jnp.float32
BF16 = jnp.bfloat16


def tile_of(extent, want):
    return want if extent % want == 0 else extent


def column_of(row):
    n = row.shape[1]
    return jnp.broadcast_to(row, (n, n)).T[:, 0:1]


def kernel(
    E, T, cap, tok_h, gain_h, logit_h, ids_h, act_h, gw_h, uw_h, dw_h, out_h,
    tok_v, gain_v, logit_v, ids_v, act_v, gw_v, uw_v, dw_v,
    ssbuf, sendbuf, x_v, gacc, uacc, hid, dsend, drecv, osum, csend, rbuf, eo, ret, hot, outbuf,
    in_sem, w_sem, ss_send, ss_recv, z_send, z_recv, p_send, p_recv, s_send, s_recv,
    d_send, d_recv, c_send, c_recv, r_send, r_recv,
):
    e = lax.axis_index("expert")
    t = lax.axis_index("tp")
    C = T // 2
    chip = t // 2
    c = lax.rem(t, 2)
    other = 1 - c
    sib = chip * 2 + other
    n, F = tok_v.shape
    ff = hid.shape[1]
    D = T * F
    rows = E * cap
    order = sorted(range(E), key=lambda d: (min(d, E - d), d))

    def group(d):
        return lax.rem(e + d, E)

    def chip_at(rel):
        return lax.rem(chip + rel + C, C)

    def grows(g):
        return pl.ds(pl.multiple_of(g * cap, cap), cap)

    def half(core):
        return pl.ds(pl.multiple_of(core * F, F), F)

    def remote(src, dst, ssem, rsem, expert, tp):
        return pltpu.make_async_remote_copy(
            src_ref=src, dst_ref=dst, send_sem=ssem, recv_sem=rsem,
            device_id=(expert, tp), device_id_type=pl.DeviceIdType.MESH)

    barrier = pltpu.get_barrier_semaphore()
    for k in range(1, T):
        pl.semaphore_signal(barrier, inc=1, device_id=(e, lax.rem(t + k, T)),
                            device_id_type=pl.DeviceIdType.MESH)
    for d in range(1, E):
        pl.semaphore_signal(barrier, inc=1, device_id=(group(d), t),
                            device_id_type=pl.DeviceIdType.MESH)

    small = [
        pltpu.make_async_copy(tok_h, tok_v, in_sem.at[0]),
        pltpu.make_async_copy(gain_h, gain_v, in_sem.at[1]),
        pltpu.make_async_copy(logit_h, logit_v, in_sem.at[2]),
        pltpu.make_async_copy(ids_h, ids_v, in_sem.at[3]),
        pltpu.make_async_copy(act_h, act_v, in_sem.at[4]),
    ]
    for cp in small:
        cp.start()
    gate_cp, up_cp = [], []
    for rel in range(C):
        q = chip_at(-rel)
        cols = pl.ds(pl.multiple_of(q * 2 * F, 2 * F), 2 * F)
        gate_cp.append(pltpu.make_async_copy(gw_h.at[0, :, cols], gw_v.at[rel], w_sem.at[0, rel]))
        up_cp.append(pltpu.make_async_copy(uw_h.at[0, :, cols], uw_v.at[rel], w_sem.at[1, rel]))
        gate_cp[-1].start()
        up_cp[-1].start()
    down_cp = {}
    down_order = list(range(1, C)) + [0]
    for rel in down_order:
        q = chip_at(rel)
        pair = []
        for i, core in enumerate((other, c)):
            cols = pl.ds(pl.multiple_of((q * 2 + core) * F, F), F)
            pair.append(pltpu.make_async_copy(dw_h.at[0, :, cols], dw_v.at[rel, i], w_sem.at[2 + i, rel]))
            pair[-1].start()
        down_cp[rel] = pair
    for cp in small:
        cp.wait()

    wide = tok_v[...].astype(F32)
    part = jnp.sum(wide * wide, axis=1, keepdims=True)
    ssbuf[t] = jnp.broadcast_to(part, (n, n)).T[0:8, :]

    ids = ids_v[...]
    active = column_of(act_v[...].astype(F32))
    lane = lax.broadcasted_iota(jnp.int32, (n, 128), 1)
    hits = ((ids[:, 0:1] == lane) | (ids[:, 1:2] == lane)).astype(F32) * active
    lower = (lax.broadcasted_iota(jnp.int32, (n, n), 0)
             > lax.broadcasted_iota(jnp.int32, (n, n), 1)).astype(F32).astype(BF16)
    position = jnp.dot(lower, hits.astype(BF16), preferred_element_type=F32)
    seat = position + (lane * cap).astype(F32)
    slot = lax.broadcasted_iota(jnp.int32, (n, rows), 1).astype(F32)
    both = jnp.zeros((n, rows), F32)
    for k in range(2):
        place = jnp.sum(jnp.where(ids[:, k:k + 1] == lane, seat, 0.0), axis=1, keepdims=True)
        place = jnp.where(active > 0.0, place, -1.0)
        one = (slot == place).astype(F32)
        hot[k] = one.astype(BF16)
        both = both + one
    pick = both.T.astype(BF16)

    pl.semaphore_wait(barrier, T - 1 + E - 1)
    ss_cp = []
    for k in range(1, T):
        ss_cp.append(remote(ssbuf.at[t], ssbuf.at[t], ss_send.at[k], ss_recv.at[k], e, lax.rem(t + k, T)))
        ss_cp[-1].start()
    for cp in ss_cp:
        cp.wait()
    total = ssbuf[0]
    for k in range(1, T):
        total = total + ssbuf[k]
    mean_square = column_of(total[0:1, :]) / D
    gain = gain_v[:, pl.ds(pl.multiple_of(t * F, F), F)].astype(F32)
    normed = (tok_v[...].astype(F32) * lax.rsqrt(mean_square + epsilon) * gain).astype(BF16)
    picked = jnp.dot(pick, normed, preferred_element_type=F32).astype(BF16)
    sendbuf[...] = picked.reshape(E, cap, F)
    x_v[chip, grows(e), half(c)] = sendbuf[e]

    z_cp = []
    for d in order[1:]:
        z_cp.append(remote(sendbuf.at[group(d)], x_v.at[chip, grows(e), half(c)],
                           z_send.at[d], z_recv.at[E - d], group(d), t))
        z_cp[-1].start()

    def block(q, d, core):
        return x_v.at[q, grows(group(d)), half(core)]

    plane = {}
    across = {}

    def forward(rel, d):
        ref = block(chip_at(-rel), d, c)
        across[rel, d] = remote(ref, ref, s_send.at[rel, d], s_recv.at[rel, d], e, sib)
        across[rel, d].start()

    for d in order:
        if d:
            remote(sendbuf.at[0], block(chip, d, c), z_send.at[d], z_recv.at[d], e, t).wait_recv()
        for rel in range(1, C):
            ref = block(chip, d, c)
            plane[rel, d] = remote(ref, ref, p_send.at[rel, d], p_recv.at[rel, d], e, chip_at(rel) * 2 + c)
            plane[rel, d].start()
        forward(0, d)

    def arrived(rel):
        for d in order:
            plane[rel, d].wait_recv()
            forward(rel, d)

    ft = tile_of(ff, 256)

    def project(rel):
        for d in order:
            across[rel, d].wait_recv()
        gate_cp[rel].wait()
        up_cp[rel].wait()
        q = chip_at(-rel)

        def step(i, carry):
            fs = pl.ds(pl.multiple_of(i * ft, ft), ft)
            x = x_v[q]
            nt = (((1,), (1,)), ((), ()))
            g = lax.dot_general(x, gw_v[rel, fs, :], nt, preferred_element_type=F32)
            u = lax.dot_general(x, uw_v[rel, fs, :], nt, preferred_element_type=F32)
            if rel > 0:
                g = gacc[i] + g
                u = uacc[i] + u
            if rel < C - 1:
                gacc[i] = g
                uacc[i] = u
            else:
                hid[:, fs] = (g / (1.0 + jnp.exp(-g)) * u).astype(BF16)
            return carry

        lax.fori_loop(0, ff // ft, step, 0)

    if C > 1:
        project(0)
        arrived(1)
        for rel in range(2, C):
            arrived(rel)
            project(rel - 1)
        project(C - 1)
    else:
        project(0)

    over = {}
    chips = {}
    back = order[::-1]

    def lower_half(rel, i, dst):
        ct = tile_of(F, 256)

        def step(j, carry):
            cs = pl.ds(pl.multiple_of(j * ct, ct), ct)
            y = jnp.dot(hid[...], dw_v[rel, i, :, cs], preferred_element_type=F32)
            dst[rel, :, cs] = y.astype(dst.dtype)
            return carry

        lax.fori_loop(0, F // ct, step, 0)

    def chip_sum(rel):
        over[rel].wait_recv()
        csend[rel] = osum[rel] + drecv[rel]
        for d in back:
            chips[rel, d] = remote(csend.at[rel, grows(group(d))], rbuf.at[rel, grows(group(d))],
                                   c_send.at[rel, d], c_recv.at[rel, d], e, chip_at(rel) * 2 + c)
            chips[rel, d].start()

    waiting = None
    for rel in down_order:
        down_cp[rel][0].wait()
        lower_half(rel, 0, dsend)
        over[rel] = remote(dsend.at[rel], drecv.at[rel], d_send.at[rel], d_recv.at[rel], e, sib)
        over[rel].start()
        down_cp[rel][1].wait()
        lower_half(rel, 1, osum)
        if waiting is not None:
            chip_sum(waiting)
        waiting = rel
    over[0].wait_recv()

    home = {}
    for d in back:
        gr = grows(group(d))
        acc = osum[0, gr, :] + drecv[0, gr, :].astype(F32)
        for rel in range(1, C):
            chips[rel, d].wait_recv()
            acc = acc + rbuf[rel, gr, :].astype(F32)
        eo[d] = acc.astype(BF16)
        if d:
            home[d] = remote(eo.at[d], ret.at[grows(e)], r_send.at[d], r_recv.at[E - d], group(d), t)
            home[d].start()
        else:
            ret[grows(e), :] = eo[0]
    logits = logit_v[...]
    first, second = logits[:, 0:1], logits[:, 1:2]
    top = jnp.maximum(first, second)
    ea, eb = jnp.exp(first - top), jnp.exp(second - top)
    scale = active / (ea + eb)
    for d in order[1:]:
        remote(eo.at[d], ret.at[grows(group(d))], r_send.at[d], r_recv.at[d], e, t).wait_recv()
    final = ret[...]
    mixed = (ea * scale) * jnp.dot(hot[0], final, preferred_element_type=F32)
    mixed = mixed + (eb * scale) * jnp.dot(hot[1], final, preferred_element_type=F32)
    outbuf[...] = mixed.astype(BF16)
    out_cp = pltpu.make_async_copy(outbuf, out_h, in_sem.at[0])
    out_cp.start()

    for cp in z_cp + list(plane.values()) + list(across.values()) + list(over.values()):
        cp.wait_send()
    for cp in list(chips.values()) + list(home.values()):
        cp.wait_send()
    out_cp.wait()


def shards(E, T, tokens, norm_gain, route_logits, expert_ids, active, gate_weight, up_weight, down_weight):
    n, F = tokens.shape
    ff = gate_weight.shape[1]
    cap = n // 2
    C = T // 2
    rows = E * cap
    ft = tile_of(ff, 256)
    any_space = pl.BlockSpec(memory_space=pl.ANY)
    dma = pltpu.SemaphoreType.DMA
    return pl.pallas_call(
        functools.partial(kernel, E, T, cap),
        out_shape=jax.ShapeDtypeStruct((n, F), BF16),
        in_specs=[any_space] * 8,
        out_specs=any_space,
        scratch_shapes=[
            pltpu.VMEM((n, F), BF16),
            pltpu.VMEM((1, T * F), BF16),
            pltpu.VMEM((n, 2), F32),
            pltpu.VMEM((n, 2), jnp.int32),
            pltpu.VMEM((1, n), jnp.int32),
            pltpu.VMEM((C, ff, 2 * F), BF16),
            pltpu.VMEM((C, ff, 2 * F), BF16),
            pltpu.VMEM((C, 2, ff, F), BF16),
            pltpu.VMEM((T, 8, n), F32),
            pltpu.VMEM((E, cap, F), BF16),
            pltpu.VMEM((C, rows, 2 * F), BF16),
            pltpu.VMEM((ff // ft, rows, ft), F32),
            pltpu.VMEM((ff // ft, rows, ft), F32),
            pltpu.VMEM((rows, ff), BF16),
            pltpu.VMEM((C, rows, F), F32),
            pltpu.VMEM((C, rows, F), F32),
            pltpu.VMEM((C, rows, F), F32),
            pltpu.VMEM((C, rows, F), F32),
            pltpu.VMEM((C, rows, F), F32),
            pltpu.VMEM((E, cap, F), BF16),
            pltpu.VMEM((rows, F), BF16),
            pltpu.VMEM((2, n, rows), BF16),
            pltpu.VMEM((n, F), BF16),
            dma((5,)), dma((4, C)), dma((T,)), dma((T,)), dma((E,)), dma((E,)),
            dma((C, E)), dma((C, E)), dma((C, E)), dma((C, E)),
            dma((C,)), dma((C,)), dma((C, E)), dma((C, E)), dma((E,)), dma((E,)),
        ],
        compiler_params=pltpu.CompilerParams(
            collective_id=0, has_side_effects=True, vmem_limit_bytes=67043328),
    )(tokens, norm_gain.reshape(1, -1), route_logits, expert_ids, active.reshape(1, -1),
      gate_weight, up_weight, down_weight)


def solution(mesh):
    in_specs = (
        P("expert", "tp"),
        P(),
        P("expert", None),
        P("expert", None),
        P("expert"),
        P("expert", "tp", None),
        P("expert", "tp", None),
        P("expert", "tp", None),
    )
    body = functools.partial(shards, mesh.shape["expert"], mesh.shape["tp"])
    return jax.shard_map(body, mesh=mesh, in_specs=in_specs, out_specs=P("expert", "tp"), check_vma=False)
```
